32 devices in a mesh: gx: 8 (over z, y), gy: 4 (over x, core).
Axes of the slice: x: 2, y: 2, z: 4, core: 2. Of those that a mesh axis runs over, the one named last changes fastest.
Arguments:
- modes: float32 [2, 3, 96, 64, 128], P(None, None, 'gx', 'gy'), may hold values from -6 to 6
- moduli: float32 [96, 64, 128], P('gx', 'gy'), may hold values from 0.5 to 2
- pinned: int32 [96, 64, 128], P('gx', 'gy'), may hold values 0 or 1
- spectrum: float32 [3, 2], replicated, may hold values from 0.175 to 5, as said below
Outputs:
- correction: float32 [2, 3, 96, 64, 128], P(None, None, 'gx', 'gy')
The draws below stay inside these ranges and needn't reach their ends.
Inputs may be any that keep to these rules, and one draw needn't show every extreme that they name: spectrum[l] = (lower, upper) with upper from 3.5 to 5 and lower 0.05 to 0.15 times upper.
All inputs are finite; a program needn't handle non-finite values. No bound on the sum of `pinned` on one device may be relied on, other than what follows from the above.
Results may differ from the reference program's by a relative error of at most 0.0003.
Values sent between devices are 32-bit elements; how exact they have to be, the bound alone decides.
A program may use at most 128 MiB of HBM per device.

```python
import math
import jax
import jax.numpy as jnp
import numpy as np
from jax import lax

VECS = 2
DEG = 3
COARSE_DEG = 4
X = 96
Y = 64
Z = 128


def draw_spectrum(key, part):
    upper_key = jax.random.fold_in(key, 11)
    ratio_key = jax.random.fold_in(key, 23)
    top_end = jax.random.uniform(upper_key, (3,), jnp.float32, 3.5, 5.0)
    fraction = jax.random.uniform(ratio_key, (3,), jnp.float32, 0.05, 0.15)
    return jnp.stack([top_end * fraction, top_end], 1)


def place_ends(values, key, low, top_value):
    longest = values.shape.index(max(values.shape))
    spots = []
    for shift in (0, 1):
        where = [jax.random.randint(jax.random.fold_in(key, axis), (), 0, length) for axis, length in enumerate(values.shape)]
        where[longest] = (where[longest] + shift) % values.shape[longest]
        spots.append(tuple(where))
    return values.at[spots[0]].set(low).at[spots[1]].set(top_value)


def steps_of(stream_key, extent, cuts, least, high):
    def one(axis_at, parts):
        heights = jax.random.uniform(jax.random.fold_in(jax.random.fold_in(stream_key, 6), axis_at), (parts,), jnp.float32, least / len(cuts), high / len(cuts))
        return jnp.repeat(jnp.exp(heights), extent[axis_at] // parts).reshape((-1,) + (1,) * (len(extent) - axis_at - 1))

    factor_of = one(*cuts[0])
    for cut in cuts[1:]:
        factor_of = factor_of * one(*cut)
    return factor_of


def scatter_about(own_key, extent, spread, limit, split=(), kind=jnp.bfloat16):
    entries = spread * jax.random.normal(own_key, extent, jnp.float32)
    if split:
        entries = entries * steps_of(own_key, extent, split, -0.22, 0.18)
    return jnp.clip(entries, -limit, limit).astype(kind)


def setup_inputs(seed: int = 0) -> dict:
    streams_of = jax.random.split(jax.random.key(seed), 5)
    modes = scatter_about(streams_of[0], (VECS, 3, X, Y, Z), 1.0, 6.0, ((2, 8), (3, 4)), jnp.float32)
    moduli = jnp.clip(jnp.exp(math.log(2.0) - 1.3862944 * jax.random.uniform(streams_of[1], (X, Y, Z), jnp.float32) ** steps_of(streams_of[1], (X, Y, Z), ((0, 8), (1, 4)), -0.2, 0.2)), 0.5, 2.0)
    pinned = place_ends((jax.random.randint(streams_of[2], (X, Y, Z), 0, 8) < 1).astype(jnp.int32), jax.random.fold_in(streams_of[2], 1), 0, 1)
    spectrum = draw_spectrum(jax.random.fold_in(streams_of[4], 71), 0)
    return {"modes": modes, "moduli": moduli, "pinned": pinned, "spectrum": spectrum}


MU_SHEAR = 1.0
LAMBDA_BULK = 1.5
PROLONG_TABLES = {4: np.array([[1.0, 0.0, 0.0], [0.375, 0.75, -0.125], [0.0, 1.0, 0.0], [-0.125, 0.75, 0.375]], dtype=np.float32), 2: np.array([[1.0, 0.0], [0.5, 0.5]], dtype=np.float32)}
GAUSS_POINTS = [-0.9602898564975363, -0.7966664774136267, -0.5255324099163290, -0.1834346424956498, 0.1834346424956498, 0.5255324099163290, 0.7966664774136267, 0.9602898564975363]
GAUSS_WEIGHTS = [0.1012285362903763, 0.2223810344533745, 0.3137066458778873, 0.3626837833783620, 0.3626837833783620, 0.3137066458778873, 0.2223810344533745, 0.1012285362903763]


def assemble(element, degree):
    coef_table = np.zeros((degree, 2 * degree + 1))
    for residue in range(degree):
        for offset in range(-degree, degree + 1):
            target = residue + offset
            if 0 <= target <= degree:
                coef_table[residue, offset + degree] += element[residue, target]
            if residue == 0 and offset <= 0:
                coef_table[residue, offset + degree] += element[degree, degree + offset]
    return coef_table.astype(np.float32)


def basis_tables(degree):
    nodes = [float(place) / degree for place in range(degree + 1)]
    points = 0.5 * (np.array(GAUSS_POINTS) + 1.0)
    weights = 0.5 * np.array(GAUSS_WEIGHTS)
    values = np.zeros((degree + 1, points.size))
    slopes = np.zeros((degree + 1, points.size))
    for column in range(degree + 1):
        product = np.ones(points.size)
        for other in range(degree + 1):
            if other != column:
                product = product * (points - nodes[other]) / (nodes[column] - nodes[other])
        values[column] = product
        slope_sum = np.zeros(points.size)
        for skipped in range(degree + 1):
            if skipped != column:
                partial_prod = np.ones(points.size) / (nodes[column] - nodes[skipped])
                for other in range(degree + 1):
                    if other != column and other != skipped:
                        partial_prod = partial_prod * (points - nodes[other]) / (nodes[column] - nodes[other])
                slope_sum = slope_sum + partial_prod
        slopes[column] = slope_sum
    mass_el = (values * weights) @ values.T
    stiff_el = (slopes * weights) @ slopes.T
    mixed_el = (slopes * weights) @ values.T
    return [assemble(mass_el, degree), assemble(stiff_el, degree), assemble(mixed_el, degree), assemble(mixed_el.T, degree)]


def coupling():
    return MU_SHEAR + (LAMBDA_BULK + MU_SHEAR) * np.eye(3, dtype=np.float32)


def line_apply(field, along, coef_table, margin):
    degree = coef_table.shape[0]
    length = field.shape[along] - 2 * degree
    residue = (np.arange(length) + degree - margin) % degree
    coef_rows = coef_table[residue]
    shape_out = [1] * field.ndim
    shape_out[along] = length
    summed = None
    for offset in range(2 * degree + 1):
        window = lax.slice_in_dim(field, offset, offset + length, 1, along)
        weighted = window * jnp.asarray(coef_rows[:, offset].reshape(shape_out))
        summed = weighted if summed is None else summed + weighted
    return summed


def z_line(field, coef_table):
    degree = coef_table.shape[0]
    widths = [(0, 0)] * (field.ndim - 1) + [(degree, degree)]
    return line_apply(jnp.pad(field, widths), field.ndim - 1, coef_table, degree)


def elastic(padded, tables, margin):
    mass_tab, stiff_tab, mixed_tab, trans_tab = tables
    weights = coupling()
    z_mass = z_line(padded, mass_tab)
    z_stiff = z_line(padded, stiff_tab)
    along_x = line_apply(line_apply(z_mass, 3, mass_tab, margin), 2, stiff_tab, margin)
    along_y = line_apply(line_apply(z_mass, 3, stiff_tab, margin), 2, mass_tab, margin)
    along_z = line_apply(line_apply(z_stiff, 3, mass_tab, margin), 2, mass_tab, margin)
    outputs = []
    for target in range(3):
        result = weights[target, 0] * along_x[:, target] + weights[target, 1] * along_y[:, target] + weights[target, 2] * along_z[:, target]
        for source in range(3):
            if source != target:
                chosen = [mass_tab, mass_tab, mass_tab]
                chosen[target] = mixed_tab
                chosen[source] = trans_tab
                coupled = z_line(padded[:, source], chosen[2])
                coupled = line_apply(coupled, 2, chosen[1], margin)
                coupled = line_apply(coupled, 1, chosen[0], margin)
                result = result + (LAMBDA_BULK + MU_SHEAR) * coupled
        outputs.append(result)
    return jnp.stack(outputs, 1)


def level_fields(moduli, pinned, stride):
    sampled = moduli[::stride, ::stride, ::stride]
    pinned_f = pinned[::stride, ::stride, ::stride].astype(jnp.float32)
    return sampled * (1.0 - pinned_f), pinned_f


def inverse_diag(scaling, pinned_f, tables):
    mass_tab, stiff_tab = tables[0], tables[1]
    degree = mass_tab.shape[0]
    weights = coupling()
    centers = []
    for along in range(3):
        residue = np.arange(scaling.shape[along]) % degree
        shape_out = [1, 1, 1]
        shape_out[along] = scaling.shape[along]
        centers.append((mass_tab[residue, degree].reshape(shape_out), stiff_tab[residue, degree].reshape(shape_out)))
    rows_out = []
    for target in range(3):
        diagonal = weights[target, 0] * centers[0][1] * centers[1][0] * centers[2][0]
        diagonal = diagonal + weights[target, 1] * centers[0][0] * centers[1][1] * centers[2][0]
        diagonal = diagonal + weights[target, 2] * centers[0][0] * centers[1][0] * centers[2][1]
        rows_out.append(scaling * scaling * jnp.asarray(diagonal) + pinned_f)
    return 1.0 / jnp.stack(rows_out, 0)


def operate(field, scaling, pinned_f, tables, padder):
    degree = tables[0].shape[0]
    padded = padder(scaling * field, degree)
    return scaling * elastic(padded, tables, degree) + pinned_f * field


def chebyshev(source, initial, n_steps, bounds, inverse, apply_op):
    low_end = bounds[0]
    top_end = bounds[1]
    center = 0.5 * (top_end + low_end)
    radius = 0.5 * (top_end - low_end)
    ratio_cs = center / radius
    rho_now = 1.0 / ratio_cs
    residual = source if initial is None else source - apply_op(initial)
    update = inverse * residual / center
    solution = update if initial is None else initial + update
    for sweep_at in range(n_steps - 1):
        residual = residual - apply_op(update)
        rho_next = 1.0 / (2.0 * ratio_cs - rho_now)
        update = rho_next * rho_now * update + (2.0 * rho_next / radius) * inverse * residual
        solution = solution + update
        rho_now = rho_next
    return solution


def alternate(pieces, along):
    stacked = jnp.stack(pieces, along + 1)
    dims_now = list(stacked.shape)
    merged = dims_now[:along] + [dims_now[along] * dims_now[along + 1]] + dims_now[along + 2:]
    return stacked.reshape(merged)


def restrict_line(field, along, table, margin):
    period, tap_count = table.shape
    half_per = period // 2
    owned_n = field.shape[along] - 2 * margin
    if margin < period:
        widths = [(0, 0)] * field.ndim
        widths[along] = (period - margin, 0)
        field = jnp.pad(field, widths)
        start_at = 0
    else:
        start_at = margin - period
    blocks = lax.slice_in_dim(field, start_at, start_at + owned_n + period, 1, along)
    dims_now = list(blocks.shape)
    elems = owned_n // period
    blocks = blocks.reshape(dims_now[:along] + [elems + 1, period] + dims_now[along + 1:])
    tap_sums = []
    for tap_at in range(tap_count):
        running = None
        for residue in range(period):
            if table[residue, tap_at] != 0.0:
                portion = float(table[residue, tap_at]) * lax.index_in_dim(blocks, residue, along + 1, False)
                running = portion if running is None else running + portion
        tap_sums.append(running)
    leading = lax.slice_in_dim(tap_sums[0], 1, elems + 1, 1, along) + lax.slice_in_dim(tap_sums[half_per], 0, elems, 1, along)
    pieces = [leading] + [lax.slice_in_dim(tap_sums[tap_at], 1, elems + 1, 1, along) for tap_at in range(1, half_per)]
    return alternate(pieces, along)


def restrict_all(field, margin, degree):
    table = PROLONG_TABLES[degree]
    coarse = restrict_line(field, 2, table, margin)
    coarse = restrict_line(coarse, 3, table, margin)
    return restrict_line(coarse, 4, table, 0)


def prolong_line(field, along, table, margin):
    period, tap_count = table.shape
    half_per = period // 2
    elems = (field.shape[along] - 2 * margin) // half_per
    columns = [lax.slice_in_dim(field, margin + tap_at, margin + tap_at + half_per * (elems - 1) + 1, half_per, along) for tap_at in range(tap_count)]
    pieces = []
    for residue in range(period):
        running = None
        for tap_at in range(tap_count):
            if table[residue, tap_at] != 0.0:
                portion = float(table[residue, tap_at]) * columns[tap_at]
                running = portion if running is None else running + portion
        pieces.append(running)
    return alternate(pieces, along)


def prolong_all(field, degree):
    table = PROLONG_TABLES[degree]
    fine = prolong_line(field, 2, table, 1)
    fine = prolong_line(fine, 3, table, 1)
    fine = jnp.pad(fine, [(0, 0)] * 4 + [(1, 1)])
    return prolong_line(fine, 4, table, 1)


def zero_pad(field, width):
    widths = [(0, 0)] * field.ndim
    widths[-3] = (width, width)
    widths[-2] = (width, width)
    return jnp.pad(field, widths)


def reference(modes, moduli, pinned, spectrum):
    degrees = [4, 2, 1]
    tables = [basis_tables(degree) for degree in degrees]
    fields = [level_fields(moduli, pinned, stride) for stride in (1, 2, 4)]

    def v_cycle(level_at, source):
        scaling, pinned_f = fields[level_at]
        inverse = inverse_diag(scaling, pinned_f, tables[level_at])[None]

        def apply_op(field):
            return operate(field, scaling, pinned_f, tables[level_at], zero_pad)

        if level_at == 2:
            return chebyshev(source, None, COARSE_DEG, spectrum[2], inverse, apply_op)
        degree = degrees[level_at]
        solution = chebyshev(source, None, DEG, spectrum[level_at], inverse, apply_op)
        residual = (1.0 - pinned_f) * source - scaling * elastic(zero_pad(scaling * solution, degree), tables[level_at], degree)
        coarse_fixed = fields[level_at + 1][1]
        coarse_src = (1.0 - coarse_fixed) * restrict_all(zero_pad(residual, degree - 1), degree - 1, degree)
        lifted = v_cycle(level_at + 1, coarse_src)
        solution = solution + (1.0 - pinned_f) * prolong_all(zero_pad(lifted, 1), degree)
        return chebyshev(source, solution, DEG, spectrum[level_at], inverse, apply_op)

    return v_cycle(0, modes)
```

```python
import functools

import jax
import jax.numpy as jnp
import numpy as np
from jax import lax
from jax.experimental import pallas as pl
from jax.experimental.pallas import tpu as pltpu
from jax.sharding import PartitionSpec as P

DEG = 3
COARSE_DEG = 4
DEGREES = (4, 2, 1)
MU_SHEAR = 1.0
LAMBDA_BULK = 1.5
PROLONG_TABLES = {
    4: np.array(
        [[1.0, 0.0, 0.0], [0.375, 0.75, -0.125], [0.0, 1.0, 0.0], [-0.125, 0.75, 0.375]]
    ),
    2: np.array([[1.0, 0.0], [0.5, 0.5]]),
}
DIRS = ((-1, 0), (0, -1), (1, 0), (0, 1), (-1, -1), (-1, 1), (1, -1), (1, 1))
F32 = jnp.float32
BF16 = jnp.bfloat16


def assemble(element, degree):
    table = np.zeros((degree, 2 * degree + 1))
    for residue in range(degree):
        for offset in range(-degree, degree + 1):
            target = residue + offset
            if 0 <= target <= degree:
                table[residue, offset + degree] += element[residue, target]
            if residue == 0 and offset <= 0:
                table[residue, offset + degree] += element[degree, degree + offset]
    return table


def basis_tables(degree):
    nodes = [float(place) / degree for place in range(degree + 1)]
    gauss_x, gauss_w = np.polynomial.legendre.leggauss(8)
    points = 0.5 * (gauss_x + 1.0)
    weights = 0.5 * gauss_w
    values = np.zeros((degree + 1, points.size))
    slopes = np.zeros((degree + 1, points.size))
    for column in range(degree + 1):
        product = np.ones(points.size)
        for other in range(degree + 1):
            if other != column:
                product = product * (points - nodes[other]) / (nodes[column] - nodes[other])
        values[column] = product
        for skipped in range(degree + 1):
            if skipped != column:
                part = np.ones(points.size) / (nodes[column] - nodes[skipped])
                for other in range(degree + 1):
                    if other != column and other != skipped:
                        part = part * (points - nodes[other]) / (nodes[column] - nodes[other])
                slopes[column] += part
    mass = (values * weights) @ values.T
    stiff = (slopes * weights) @ slopes.T
    mixed = (slopes * weights) @ values.T
    return [assemble(e, degree) for e in (mass, stiff, mixed, mixed.T)]


def dense(table, count):
    p = table.shape[0]
    out = np.zeros((count, count + p + 1))
    for i in range(count):
        for o in range(-p, p + 1):
            c = table[i % p, o + p]
            if c != 0.0 and i + o <= count:
                out[i, i + o + p] += c
    return out


def up8(n):
    return -(-n // 8) * 8


class Level:
    def __init__(self, degree, nx, ny, nz, vecs):
        p = self.p = degree
        self.nx, self.ny, self.nz, self.vecs = nx, ny, nz, vecs
        self.own = nx * ny
        self.rows = up8(self.own)
        self.lanes = -(-vecs * nz // 128) * 128
        self.pos = [(x, y) for x in range(nx) for y in range(ny)]
        self.pos += [None] * (self.rows - self.own)
        self.blocks = []
        self.halo_pos = []
        for dx, dy in DIRS:
            src_x = {-1: range(nx - p, nx), 0: range(nx), 1: range(1)}[dx]
            src_y = {-1: range(ny - p, ny), 0: range(ny), 1: range(1)}[dy]
            start = len(self.halo_pos)
            runs = []
            for x in src_x:
                at = len(self.halo_pos)
                runs.append((at, x * ny + src_y[0], len(src_y)))
                self.halo_pos += [(x + dx * nx, y + dy * ny) for y in src_y]
            merged = [runs[0]]
            for run in runs[1:]:
                a, b, n = merged[-1]
                if run[0] == a + n and run[1] == b + n:
                    merged[-1] = (a, b, n + run[2])
                else:
                    merged.append(run)
            size = up8(len(self.halo_pos) - start)
            self.halo_pos += [None] * (start + size - len(self.halo_pos))
            self.blocks.append((start, size, merged))
        self.halo = len(self.halo_pos)

    def plane(self, mat_x, mat_y, rows_out, positions):
        out = np.zeros((rows_out, len(positions)))
        for k, at in enumerate(positions):
            if at is not None:
                col = np.outer(mat_x[:, at[0] + self.p], mat_y[:, at[1] + self.p]).ravel()
                out[: col.size, k] = col
        return out

    def operator(self):
        t = basis_tables(self.p)
        m_x, k_x, g_x, t_x = [dense(e, self.nx) for e in t]
        m_y, k_y, g_y, t_y = [dense(e, self.ny) for e in t]
        cc = LAMBDA_BULK + MU_SHEAR
        big = MU_SHEAR + cc
        groups = [
            [((big, k_x, m_y), (MU_SHEAR, m_x, k_y)), ((1, m_x, m_y),), ((cc, t_x, g_y),), ((cc, t_x, m_y),)],
            [((MU_SHEAR, k_x, m_y), (big, m_x, k_y)), ((1, m_x, m_y),), ((cc, g_x, t_y),), ((cc, m_x, t_y),)],
            [((MU_SHEAR, k_x, m_y), (MU_SHEAR, m_x, k_y)), ((1, m_x, m_y),), ((cc, g_x, m_y),), ((cc, m_x, g_y),)],
        ]

        def build(positions):
            return np.stack(
                [
                    np.concatenate(
                        [
                            sum(w * self.plane(a, b, self.rows, positions) for w, a, b in terms)
                            for terms in source
                        ]
                    )
                    for source in groups
                ]
            )

        line = [self.lift_z(dense(e, self.nz)[:, self.p : self.p + self.nz], self) for e in t]
        z_ops = np.stack([line[0], MU_SHEAR * line[1], big * line[1], line[2], line[3]])
        return build(self.pos), build(self.halo_pos), z_ops

    def lift_z(self, mat, to):
        full = np.kron(np.eye(self.vecs), mat.T)
        out = np.zeros((self.lanes, to.lanes))
        out[: full.shape[0], : full.shape[1]] = full
        return out

    def diagonal(self):
        t = basis_tables(self.p)

        def center(table, count):
            return table[np.arange(count) % self.p, self.p]

        m = [center(t[0], n) for n in (self.nx, self.ny, self.nz)]
        k = [center(t[1], n) for n in (self.nx, self.ny, self.nz)]
        out = np.zeros((3, self.nx, self.ny, self.nz))
        for c in range(3):
            for e in range(3):
                coef = MU_SHEAR + (LAMBDA_BULK + MU_SHEAR) * (c == e)
                f = [k[i] if i == e else m[i] for i in range(3)]
                out[c] += coef * f[0][:, None, None] * f[1][None, :, None] * f[2][None, None, :]
        return out.astype(np.float32)


def prolong_dense(table, fine_n, lead):
    q = table.shape[0]
    half = q // 2
    out = np.zeros((fine_n, fine_n // 2 + lead + 1))
    for i in range(fine_n):
        for t in range(half + 1):
            j = half * (i // q) + t
            out[i, j + lead] += table[i % q, t]
    return out


def restrict_dense(table, fine_n):
    q = table.shape[0]
    half = q // 2
    out = np.zeros((fine_n // 2, fine_n + q + 1))
    for j in range(fine_n // 2):
        for i in range(-q, fine_n):
            t = j - half * (i // q)
            if 0 <= t <= half:
                out[j, i + q] += table[i % q, t]
    return out


def transfer(fine, coarse):
    table = PROLONG_TABLES[fine.p]
    rx, ry = restrict_dense(table, fine.nx), restrict_dense(table, fine.ny)
    rz = restrict_dense(table, fine.nz)[:, fine.p : fine.p + fine.nz]
    px = prolong_dense(table, fine.nx, coarse.p)
    py = prolong_dense(table, fine.ny, coarse.p)
    pz = prolong_dense(table, fine.nz, coarse.p)[:, coarse.p : coarse.p + coarse.nz]
    return (
        fine.plane(rx, ry, coarse.rows, fine.pos),
        fine.plane(rx, ry, coarse.rows, fine.halo_pos),
        fine.lift_z(rz, coarse),
        coarse.plane(px, py, fine.rows, coarse.pos),
        coarse.plane(px, py, fine.rows, coarse.halo_pos),
        coarse.lift_z(pz, fine),
    )


def split(mat):
    mat = np.asarray(mat, np.float32)
    hi = mat.astype(BF16)
    return [hi, (mat - hi.astype(np.float32)).astype(BF16)]


def halves(value):
    hi = value.astype(BF16)
    return hi, (value - hi.astype(F32)).astype(BF16)


def dot3(a, b):
    def one(u, v):
        return lax.dot_general(u, v, (((1,), (0,)), ((), ())), preferred_element_type=F32)

    return one(a[0], b[0]) + one(a[0], b[1]) + one(a[1], b[0])


def kernel(levels, names, *refs):
    R = dict(zip(names, refs))
    gx_n, gy_n = lax.axis_size("gx"), lax.axis_size("gy")
    me_x, me_y = lax.axis_index("gx"), lax.axis_index("gy")

    def reach(dx, dy):
        ok = None
        for d, me, n in ((dx, me_x, gx_n), (dy, me_y, gy_n)):
            if d:
                here = me + d < n if d > 0 else me + d >= 0
                ok = here if ok is None else jnp.logical_and(ok, here)
        return ok

    def device(dx, dy):
        return (jnp.clip(me_x + dx, 0, gx_n - 1), jnp.clip(me_y + dy, 0, gy_n - 1))

    for l, lev in enumerate(levels):
        R[f"halo{l}"][...] = jnp.zeros_like(R[f"halo{l}"])
        R[f"send{l}"][...] = jnp.zeros_like(R[f"send{l}"])
    barrier = pltpu.get_barrier_semaphore()
    for dx, dy in DIRS:

        @pl.when(reach(dx, dy))
        def _():
            pl.semaphore_signal(
                barrier, inc=1, device_id=device(dx, dy), device_id_type=pl.DeviceIdType.MESH
            )

    around = [
        1 + (me > 0).astype(jnp.int32) + (me < n - 1).astype(jnp.int32)
        for me, n in ((me_x, gx_n), (me_y, gy_n))
    ]
    pl.semaphore_wait(barrier, around[0] * around[1] - 1)

    def copies(l, slot):
        for i, (dx, dy) in enumerate(DIRS):
            start, size, _ = levels[l].blocks[i]
            yield (
                dx,
                dy,
                pltpu.make_async_remote_copy(
                    src_ref=R[f"send{l}"].at[:, pl.ds(start, size), :],
                    dst_ref=R[f"halo{l}"].at[slot, :, pl.ds(start, size), :],
                    send_sem=R[f"ssem{l}"].at[i],
                    recv_sem=R[f"rsem{l}"].at[slot, i],
                    device_id=device(-dx, -dy),
                    device_id_type=pl.DeviceIdType.MESH,
                ),
            )

    def exchange(l, slot, value):
        lev = levels[l]
        work, send = R[f"work{l}"], R[f"send{l}"]

        def stage(c, _):
            work[c] = value(c)
            for _, _, runs in lev.blocks:
                for at, src, n in runs:
                    send[c, at : at + n, :] = work[c, src : src + n, :]
            return 0

        lax.fori_loop(0, 3, stage, 0)
        for dx, dy, copy in copies(l, slot):
            pl.when(reach(-dx, -dy))(copy.start)

    def arrive(l, slot):
        for dx, dy, copy in copies(l, slot):
            pl.when(reach(dx, dy))(copy.wait_recv)
            pl.when(reach(-dx, -dy))(copy.wait_send)

    def pair(name, *at):
        return tuple(R[name + h][at] if at else R[name + h][...] for h in ("h", "l"))

    def apply_step(l, k, slot):
        lev = levels[l]
        rows = lev.rows
        s, d, r, x, prod = (R[f"{n}{l}"] for n in ("s", "d", "r", "x", "prod"))
        exchange(l, slot, lambda c: s[...] * d[c])

        def near(c, _):
            prod[c] = dot3(pair(f"wo{l}", c), halves(R[f"work{l}"][c]))
            return 0

        def far(c, _):
            prod[c] += dot3(pair(f"wh{l}", c), halves(R[f"halo{l}"][slot, c]))
            return 0

        lax.fori_loop(0, 3, near, 0)
        arrive(l, slot)
        lax.fori_loop(0, 3, far, 0)

        def group(c, g):
            return prod[c, g * rows : (g + 1) * rows, :]

        zmat = [pair(f"z{l}", i) for i in range(5)]
        parts = [
            ((group(0, 0) + group(1, 2), 0), (group(0, 1), 1), (group(2, 2), 4)),
            ((group(1, 0) + group(0, 2), 0), (group(1, 1), 1), (group(2, 3), 4)),
            ((group(2, 0), 0), (group(2, 1), 2), (group(0, 3) + group(1, 3), 3)),
        ]
        c1 = R["coef"][l, 2 * k]
        c2 = R["coef"][l, 2 * k + 1]
        for c in range(3):
            total = None
            for val, z in parts[c]:
                one = dot3(halves(val), zmat[z])
                total = one if total is None else total + one
            res = r[c] - (s[...] * total + R[f"f{l}"][...] * d[c])
            r[c] = res
            new = c1 * d[c] + c2 * (R[f"dinv{l}"][c] * res)
            d[c] = new
            x[c] += new

    def move(l, slot, value, name, out):
        exchange(l, slot, value)
        arrive(l, slot)

        def one(c, _):
            flat = dot3(pair(name + "o"), halves(R[f"work{l}"][c]))
            flat += dot3(pair(name + "h"), halves(R[f"halo{l}"][slot, c]))
            out(c, dot3(halves(flat), pair(name + "z")))
            return 0

        lax.fori_loop(0, 3, one, 0)

    def start(l, c, b):
        first = R["coef"][l, 12] * (R[f"dinv{l}"][c] * b)
        R[f"r{l}"][c] = b
        R[f"d{l}"][c] = first
        R[f"x{l}"][c] = first

    def run(l):
        last = l == len(levels) - 1

        def body(k, _):
            slot = k % 2 if last else (k + k // 3) % 2
            apply_step(l, k, slot)
            if not last:

                @pl.when(k == DEG - 1)
                def _():
                    def down(c, val):
                        start(l + 1, c, (1.0 - R[f"f{l + 1}"][...]) * val)

                    def up(c, val):
                        step = (1.0 - R[f"f{l}"][...]) * val
                        R[f"d{l}"][c] = step
                        R[f"x{l}"][c] += step

                    move(l, 1, lambda c: (1.0 - R[f"f{l}"][...]) * R[f"r{l}"][c], f"rs{l}", down)
                    run(l + 1)
                    move(l + 1, 1, lambda c: R[f"x{l + 1}"][c], f"pr{l}", up)

            return 0

        lax.fori_loop(0, COARSE_DEG - 1 if last else 2 * DEG, body, 0)

    chebyshev_table(R["spectrum"], R["coef"])
    vecs, nz = levels[0].vecs, levels[0].nz
    for c in range(3):
        for v in range(vecs):
            R["r0"][c, :, v * nz : (v + 1) * nz] = R["modes"][v, c]
        start(0, c, R["r0"][c])
    run(0)
    for c in range(3):
        for v in range(vecs):
            R["out"][v, c] = R["x0"][c, :, v * nz : (v + 1) * nz]


def chebyshev_table(spectrum, coef):
    for l in range(3):
        low, top = spectrum[l, 0], spectrum[l, 1]
        center = 0.5 * (top + low)
        radius = 0.5 * (top - low)
        ratio = center / radius
        rho = 1.0 / ratio
        steps = []
        for _ in range(COARSE_DEG - 1):
            rho_next = 1.0 / (2.0 * ratio - rho)
            steps.append((rho_next * rho, 2.0 * rho_next / radius))
            rho = rho_next
        smooth = steps[: DEG - 1]
        flat = [(0.0, 0.0), (0.0, 1.0 / center)]
        picked = steps if l == 2 else smooth + flat + smooth
        for k, two in enumerate(picked):
            coef[l, 2 * k] = jnp.asarray(two[0], F32)
            coef[l, 2 * k + 1] = jnp.asarray(two[1], F32)
        coef[l, 12] = 1.0 / center


def local(modes, moduli, pinned, spectrum):
    vecs, _, nx, ny, nz = modes.shape
    levels = []
    names, args = [], []

    def add(name, value):
        names.append(name)
        args.append(value)

    for l, degree in enumerate(DEGREES):
        step = DEGREES[0] // degree
        levels.append(Level(degree, nx // step, ny // step, nz // step, vecs))
    add("spectrum", spectrum)
    add("modes", modes.reshape(vecs, 3, nx * ny, nz))
    for l, lev in enumerate(levels):
        step = DEGREES[0] // lev.p
        w = moduli[::step, ::step, ::step]
        f = pinned[::step, ::step, ::step].astype(F32)
        s = w * (1.0 - f)
        dinv = 1.0 / (s * s * lev.diagonal() + f)

        def spread(a, fill):
            a = a.reshape(a.shape[:-3] + (lev.own, lev.nz))
            a = jnp.concatenate([a] * vecs, -1)
            wide = [(0, 0)] * (a.ndim - 2)
            wide += [(0, lev.rows - lev.own), (0, lev.lanes - vecs * lev.nz)]
            return jnp.pad(a, wide, constant_values=fill)

        add(f"s{l}", spread(s, 0.0))
        add(f"f{l}", spread(f, 1.0))
        add(f"dinv{l}", spread(dinv, 1.0))
        mats = dict(zip((f"wo{l}", f"wh{l}", f"z{l}"), lev.operator()))
        if l + 1 < len(levels):
            keys = [f"{a}{l}{b}" for a in ("rs", "pr") for b in "ohz"]
            mats.update(zip(keys, transfer(lev, levels[l + 1])))
        for key, mat in mats.items():
            for tag, half in zip("hl", split(mat)):
                add(key + tag, jnp.asarray(half))

    specs = [
        pl.BlockSpec(memory_space=pltpu.SMEM if n == "spectrum" else pltpu.VMEM) for n in names
    ]
    scratch = []
    all_names = names + ["out"]

    def temp(name, what):
        all_names.append(name)
        scratch.append(what)

    temp("coef", pltpu.SMEM((3, 13), F32))
    for l, lev in enumerate(levels):
        field = (3, lev.rows, lev.lanes)
        for n in ("r", "d", "x", "work"):
            temp(f"{n}{l}", pltpu.VMEM(field, F32))
        temp(f"prod{l}", pltpu.VMEM((3, 4 * lev.rows, lev.lanes), F32))
        temp(f"send{l}", pltpu.VMEM((3, lev.halo, lev.lanes), F32))
        temp(f"halo{l}", pltpu.VMEM((2, 3, lev.halo, lev.lanes), F32))
        temp(f"ssem{l}", pltpu.SemaphoreType.DMA((len(DIRS),)))
        temp(f"rsem{l}", pltpu.SemaphoreType.DMA((2, len(DIRS))))
    out = pl.pallas_call(
        functools.partial(kernel, levels, all_names),
        out_shape=jax.ShapeDtypeStruct((vecs, 3, nx * ny, nz), F32),
        in_specs=specs,
        out_specs=pl.BlockSpec(memory_space=pltpu.VMEM),
        scratch_shapes=scratch,
        compiler_params=pltpu.CompilerParams(
            collective_id=0, has_side_effects=True, vmem_limit_bytes=60 * 1024 * 1024
        ),
    )(*args)
    return out.reshape(modes.shape)


def solution(mesh):
    placed = (P(None, None, "gx", "gy", None), P("gx", "gy", None), P("gx", "gy", None), P())
    return jax.shard_map(
        local,
        mesh=mesh,
        in_specs=placed,
        out_specs=P(None, None, "gx", "gy", None),
        check_vma=False,
    )
```

```python
import functools

import jax
import jax.numpy as jnp
import numpy as np
from jax import lax
from jax.experimental import pallas as pl
from jax.experimental.pallas import tpu as pltpu
from jax.sharding import PartitionSpec as P

DEG = 3
COARSE_DEG = 4
DEGREES = (4, 2, 1)
MU_SHEAR = 1.0
LAMBDA_BULK = 1.5
PROLONG_TABLES = {
    4: np.array(
        [[1.0, 0.0, 0.0], [0.375, 0.75, -0.125], [0.0, 1.0, 0.0], [-0.125, 0.75, 0.375]]
    ),
    2: np.array([[1.0, 0.0], [0.5, 0.5]]),
}
DIRS = ((-1, 0), (0, -1), (1, 0), (0, 1), (-1, -1), (-1, 1), (1, -1), (1, 1))
F32 = jnp.float32
BF16 = jnp.bfloat16


def assemble(element, degree):
    table = np.zeros((degree, 2 * degree + 1))
    for residue in range(degree):
        for offset in range(-degree, degree + 1):
            target = residue + offset
            if 0 <= target <= degree:
                table[residue, offset + degree] += element[residue, target]
            if residue == 0 and offset <= 0:
                table[residue, offset + degree] += element[degree, degree + offset]
    return table


def basis_tables(degree):
    nodes = [float(place) / degree for place in range(degree + 1)]
    gauss_x, gauss_w = np.polynomial.legendre.leggauss(8)
    points = 0.5 * (gauss_x + 1.0)
    weights = 0.5 * gauss_w
    values = np.zeros((degree + 1, points.size))
    slopes = np.zeros((degree + 1, points.size))
    for column in range(degree + 1):
        product = np.ones(points.size)
        for other in range(degree + 1):
            if other != column:
                product = product * (points - nodes[other]) / (nodes[column] - nodes[other])
        values[column] = product
        for skipped in range(degree + 1):
            if skipped != column:
                part = np.ones(points.size) / (nodes[column] - nodes[skipped])
                for other in range(degree + 1):
                    if other != column and other != skipped:
                        part = part * (points - nodes[other]) / (nodes[column] - nodes[other])
                slopes[column] += part
    mass = (values * weights) @ values.T
    stiff = (slopes * weights) @ slopes.T
    mixed = (slopes * weights) @ values.T
    return [assemble(e, degree) for e in (mass, stiff, mixed, mixed.T)]


def dense(table, count):
    p = table.shape[0]
    out = np.zeros((count, count + p + 1))
    for i in range(count):
        for o in range(-p, p + 1):
            c = table[i % p, o + p]
            if c != 0.0 and i + o <= count:
                out[i, i + o + p] += c
    return out


def up8(n):
    return -(-n // 8) * 8


class Level:
    def __init__(self, degree, nx, ny, nz, vecs):
        p = self.p = degree
        self.nx, self.ny, self.nz, self.vecs = nx, ny, nz, vecs
        self.own = nx * ny
        self.rows = up8(self.own)
        self.lanes = -(-vecs * nz // 128) * 128
        self.blocked = nz % 128 == 0
        self.pos = [(x, y) for x in range(nx) for y in range(ny)]
        self.pos += [None] * (self.rows - self.own)
        self.blocks = []
        self.halo_pos = []
        for dx, dy in DIRS:
            src_x = {-1: range(nx - p, nx), 0: range(nx), 1: range(1)}[dx]
            src_y = {-1: range(ny - p, ny), 0: range(ny), 1: range(1)}[dy]
            start = len(self.halo_pos)
            runs = []
            for x in src_x:
                at = len(self.halo_pos)
                runs.append((at, x * ny + src_y[0], len(src_y)))
                self.halo_pos += [(x + dx * nx, y + dy * ny) for y in src_y]
            merged = [runs[0]]
            for run in runs[1:]:
                a, b, n = merged[-1]
                if run[0] == a + n and run[1] == b + n:
                    merged[-1] = (a, b, n + run[2])
                else:
                    merged.append(run)
            size = up8(len(self.halo_pos) - start)
            self.halo_pos += [None] * (start + size - len(self.halo_pos))
            self.blocks.append((start, size, merged))
        self.halo = len(self.halo_pos)

    def plane(self, mat_x, mat_y, rows_out, positions):
        out = np.zeros((rows_out, len(positions)))
        for k, at in enumerate(positions):
            if at is not None:
                col = np.outer(mat_x[:, at[0] + self.p], mat_y[:, at[1] + self.p]).ravel()
                out[: col.size, k] = col
        return out

    def operator(self):
        t = basis_tables(self.p)
        m_x, k_x, g_x, t_x = [dense(e, self.nx) for e in t]
        m_y, k_y, g_y, t_y = [dense(e, self.ny) for e in t]
        cc = LAMBDA_BULK + MU_SHEAR
        big = MU_SHEAR + cc
        groups = [
            [((big, k_x, m_y), (MU_SHEAR, m_x, k_y)), ((1, m_x, m_y),), ((cc, t_x, g_y),), ((cc, t_x, m_y),)],
            [((MU_SHEAR, k_x, m_y), (big, m_x, k_y)), ((1, m_x, m_y),), ((cc, g_x, t_y),), ((cc, m_x, t_y),)],
            [((MU_SHEAR, k_x, m_y), (MU_SHEAR, m_x, k_y)), ((1, m_x, m_y),), ((cc, g_x, m_y),), ((cc, m_x, g_y),)],
        ]

        def build(positions):
            return np.stack(
                [
                    np.concatenate(
                        [
                            sum(w * self.plane(a, b, self.rows, positions) for w, a, b in terms)
                            for terms in source
                        ]
                    )
                    for source in groups
                ]
            )

        line = [dense(e, self.nz)[:, self.p : self.p + self.nz] for e in t]
        line = [e.T if self.blocked else self.lift_z(e, self) for e in line]
        z_ops = np.stack([line[0], MU_SHEAR * line[1], big * line[1], line[2], line[3]])
        return build(self.pos), build(self.halo_pos), z_ops

    def lift_z(self, mat, to):
        full = np.kron(np.eye(self.vecs), mat.T)
        out = np.zeros((self.lanes, to.lanes))
        out[: full.shape[0], : full.shape[1]] = full
        return out

    def diagonal(self):
        t = basis_tables(self.p)

        def center(table, count):
            return table[np.arange(count) % self.p, self.p]

        m_x, m_y, m_z = [center(t[0], n) for n in (self.nx, self.ny, self.nz)]
        k_x, k_y, k_z = [center(t[1], n) for n in (self.nx, self.ny, self.nz)]
        rows = np.zeros((self.rows, 128), np.float32)
        for c in range(3):
            coef = [MU_SHEAR + (LAMBDA_BULK + MU_SHEAR) * (c == e) for e in range(3)]
            plane = coef[0] * np.outer(k_x, m_y) + coef[1] * np.outer(m_x, k_y)
            rows[: self.own, c] = plane.ravel()
            rows[: self.own, 3 + c] = (coef[2] * np.outer(m_x, m_y)).ravel()
        lanes = np.zeros((8, self.lanes), np.float32)
        lanes[0, : self.vecs * self.nz] = np.tile(m_z, self.vecs)
        lanes[1, : self.vecs * self.nz] = np.tile(k_z, self.vecs)
        return rows, lanes

    def sample(self, top):
        step = top.p // self.p
        sel_x = np.zeros((self.rows, top.own))
        for i, (x, y) in enumerate(self.pos[: self.own]):
            sel_x[i, x * step * top.ny + y * step] = 1
        sel_z = np.zeros((top.nz, self.lanes))
        for v in range(self.vecs):
            for z in range(self.nz):
                sel_z[z * step, v * self.nz + z] = 1
        return sel_x, sel_z


def prolong_dense(table, fine_n, lead):
    q = table.shape[0]
    half = q // 2
    out = np.zeros((fine_n, fine_n // 2 + lead + 1))
    for i in range(fine_n):
        for t in range(half + 1):
            j = half * (i // q) + t
            out[i, j + lead] += table[i % q, t]
    return out


def restrict_dense(table, fine_n):
    q = table.shape[0]
    half = q // 2
    out = np.zeros((fine_n // 2, fine_n + q + 1))
    for j in range(fine_n // 2):
        for i in range(-q, fine_n):
            t = j - half * (i // q)
            if 0 <= t <= half:
                out[j, i + q] += table[i % q, t]
    return out


def transfer(fine, coarse):
    table = PROLONG_TABLES[fine.p]
    rx, ry = restrict_dense(table, fine.nx), restrict_dense(table, fine.ny)
    rz = restrict_dense(table, fine.nz)[:, fine.p : fine.p + fine.nz]
    px = prolong_dense(table, fine.nx, coarse.p)
    py = prolong_dense(table, fine.ny, coarse.p)
    pz = prolong_dense(table, fine.nz, coarse.p)[:, coarse.p : coarse.p + coarse.nz]
    return (
        fine.plane(rx, ry, coarse.rows, fine.pos),
        fine.plane(rx, ry, coarse.rows, fine.halo_pos),
        fine.lift_z(rz, coarse),
        coarse.plane(px, py, fine.rows, coarse.pos),
        coarse.plane(px, py, fine.rows, coarse.halo_pos),
        coarse.lift_z(pz, fine),
    )


def split(mat):
    mat = np.asarray(mat, np.float32)
    hi = mat.astype(BF16)
    return [hi, (mat - hi.astype(np.float32)).astype(BF16)]


def halves(value):
    hi = value.astype(BF16)
    return hi, (value - hi.astype(F32)).astype(BF16)


def dot3(a, b):
    def one(u, v):
        return lax.dot_general(u, v, (((1,), (0,)), ((), ())), preferred_element_type=F32)

    return one(a[0], b[0]) + one(a[0], b[1]) + one(a[1], b[0])


def kernel(levels, names, *refs):
    R = dict(zip(names, refs))
    gx_n, gy_n = lax.axis_size("gx"), lax.axis_size("gy")
    me_x, me_y = lax.axis_index("gx"), lax.axis_index("gy")

    def reach(dx, dy):
        ok = None
        for d, me, n in ((dx, me_x, gx_n), (dy, me_y, gy_n)):
            if d:
                here = me + d < n if d > 0 else me + d >= 0
                ok = here if ok is None else jnp.logical_and(ok, here)
        return ok

    def device(dx, dy):
        return (jnp.clip(me_x + dx, 0, gx_n - 1), jnp.clip(me_y + dy, 0, gy_n - 1))

    top = levels[0]
    vecs, nz = top.vecs, top.nz
    if top.blocked:
        for h in "hl":
            R[f"z0{h}"][...] = jnp.zeros_like(R[f"z0{h}"])
    moves = [(R["moduli_in"], R["moduli"]), (R["pinned_in"], R["pinned"])]
    for v in range(vecs):
        moves.append((R["modes"].at[v], R["r0"].at[:, :, pl.ds(v * nz, nz)]))
    for name in names:
        if name.endswith("_in") and name[:-3] not in ("moduli", "pinned"):
            src, dst = R[name], R[name[:-3]]
            if name[:2] == "z0" and top.blocked:
                for v in range(vecs):
                    at = pl.ds(v * nz, nz)
                    moves.append((src, dst.at[:, at, at]))
            else:
                moves.append((src, dst))
    moves = [
        pltpu.make_async_copy(src, dst, R["lsem"].at[i]) for i, (src, dst) in enumerate(moves)
    ]
    for one in moves:
        one.start()
    chebyshev_table(R["spectrum"], R["coef"])
    for l, lev in enumerate(levels):
        R[f"halo{l}"][...] = jnp.zeros_like(R[f"halo{l}"])
        R[f"send{l}"][...] = jnp.zeros_like(R[f"send{l}"])
    barrier = pltpu.get_barrier_semaphore()
    for dx, dy in DIRS:

        @pl.when(reach(dx, dy))
        def _():
            pl.semaphore_signal(
                barrier, inc=1, device_id=device(dx, dy), device_id_type=pl.DeviceIdType.MESH
            )

    around = [
        1 + (me > 0).astype(jnp.int32) + (me < n - 1).astype(jnp.int32)
        for me, n in ((me_x, gx_n), (me_y, gy_n))
    ]
    pl.semaphore_wait(barrier, around[0] * around[1] - 1)

    def copies(l, slot, side):
        for i, (dx, dy) in enumerate(DIRS):
            if side and -side in (dx, dy):
                continue
            start, size, _ = levels[l].blocks[i]
            yield (
                dx,
                dy,
                pltpu.make_async_remote_copy(
                    src_ref=R[f"send{l}"].at[:, pl.ds(start, size), :],
                    dst_ref=R[f"halo{l}"].at[slot, :, pl.ds(start, size), :],
                    send_sem=R[f"ssem{l}"].at[i],
                    recv_sem=R[f"rsem{l}"].at[slot, i],
                    device_id=device(-dx, -dy),
                    device_id_type=pl.DeviceIdType.MESH,
                ),
            )

    def exchange(l, slot, value, side=0):
        lev = levels[l]
        work, send = R[f"work{l}"], R[f"send{l}"]

        def stage(c, _):
            work[c] = value(c)
            for _, _, runs in lev.blocks:
                for at, src, n in runs:
                    send[c, at : at + n, :] = work[c, src : src + n, :]
            return 0

        lax.fori_loop(0, 3, stage, 0)
        for dx, dy, copy in copies(l, slot, side):
            pl.when(reach(-dx, -dy))(copy.start)

    def arrive(l, slot, side=0):
        for dx, dy, copy in copies(l, slot, side):
            pl.when(reach(dx, dy))(copy.wait_recv)
            pl.when(reach(-dx, -dy))(copy.wait_send)

    def pair(name, *at):
        return tuple(R[name + h][at] if at else R[name + h][...] for h in ("h", "l"))

    def apply_step(l, k, slot):
        lev = levels[l]
        rows = lev.rows
        s, d, r, x, prod = (R[f"{n}{l}"] for n in ("s", "d", "r", "x", "prod"))
        exchange(l, slot, lambda c: s[...] * d[c])

        def near(c, _):
            prod[c] = dot3(pair(f"wo{l}", c), halves(R[f"work{l}"][c]))
            return 0

        def far(c, _):
            prod[c] += dot3(pair(f"wh{l}", c), halves(R[f"halo{l}"][slot, c]))
            return 0

        lax.fori_loop(0, 3, near, 0)
        arrive(l, slot)
        lax.fori_loop(0, 3, far, 0)

        def group(c, g):
            return prod[c, g * rows : (g + 1) * rows, :]

        zmat = [pair(f"z{l}", i) for i in range(5)]
        parts = [
            ((group(0, 0) + group(1, 2), 0), (group(0, 1), 1), (group(2, 2), 4)),
            ((group(1, 0) + group(0, 2), 0), (group(1, 1), 1), (group(2, 3), 4)),
            ((group(2, 0), 0), (group(2, 1), 2), (group(0, 3) + group(1, 3), 3)),
        ]
        c1 = R["coef"][l, 2 * k]
        c2 = R["coef"][l, 2 * k + 1]
        for c in range(3):
            total = None
            for val, z in parts[c]:
                one = dot3(halves(val), zmat[z])
                total = one if total is None else total + one
            res = r[c] - (s[...] * total + R[f"f{l}"][...] * d[c])
            r[c] = res
            new = c1 * d[c] + c2 * (R[f"dinv{l}"][c] * res)
            d[c] = new
            x[c] += new

    def move(l, slot, value, name, out, side):
        exchange(l, slot, value, side)
        arrive(l, slot, side)

        def one(c, _):
            flat = dot3(pair(name + "o"), halves(R[f"work{l}"][c]))
            flat += dot3(pair(name + "h"), halves(R[f"halo{l}"][slot, c]))
            out(c, dot3(halves(flat), pair(name + "z")))
            return 0

        lax.fori_loop(0, 3, one, 0)

    def start(l, c, b):
        first = R["coef"][l, 12] * (R[f"dinv{l}"][c] * b)
        R[f"r{l}"][c] = b
        R[f"d{l}"][c] = first
        R[f"x{l}"][c] = first

    def run(l):
        last = l == len(levels) - 1

        def body(k, _):
            slot = k % 2 if last else (k + k // 3) % 2
            apply_step(l, k, slot)
            if not last:

                @pl.when(k == DEG - 1)
                def _():
                    def down(c, val):
                        start(l + 1, c, (1.0 - R[f"f{l + 1}"][...]) * val)

                    def up(c, val):
                        step = (1.0 - R[f"f{l}"][...]) * val
                        R[f"d{l}"][c] = step
                        R[f"x{l}"][c] += step

                    move(l, 1, lambda c: (1.0 - R[f"f{l}"][...]) * R[f"r{l}"][c], f"rs{l}", down, -1)
                    run(l + 1)
                    move(l + 1, 1, lambda c: R[f"x{l + 1}"][c], f"pr{l}", up, 1)

            return 0

        lax.fori_loop(0, COARSE_DEG - 1 if last else 2 * DEG, body, 0)

    for one in moves:
        one.wait()
    free = 1.0 - R["pinned"][...].astype(F32)
    scale = R["moduli"][...] * free

    def times01(a, b):
        return lax.dot_general(a, b, (((1,), (0,)), ((), ())), preferred_element_type=F32)

    def thirds(value):
        hi, lo = halves(value)
        rest = value - hi.astype(F32) - lo.astype(F32)
        return hi, lo, rest.astype(BF16)

    for l, lev in enumerate(levels):
        if l == 0 and lev.blocked:
            for v in range(vecs):
                at = pl.ds(v * nz, nz)
                R["s0"][:, at] = scale
                R["f0"][:, at] = 1.0 - free
        else:
            sel_x, sel_z = R[f"sx{l}"][...], R[f"sz{l}"][...]
            picked = sum(times01(sel_x, part) for part in thirds(scale))
            R[f"s{l}"][...] = sum(times01(part, sel_z) for part in thirds(picked))
            picked = times01(sel_x, free.astype(BF16))
            R[f"f{l}"][...] = 1.0 - times01(picked.astype(BF16), sel_z)
        square = R[f"s{l}"][...] * R[f"s{l}"][...]
        m_z, k_z = R[f"kl{l}"][0:1, :], R[f"kl{l}"][1:2, :]
        for c in range(3):
            kd = R[f"kr{l}"][:, c : c + 1] * m_z + R[f"kr{l}"][:, 3 + c : 4 + c] * k_z
            R[f"dinv{l}"][c] = 1.0 / (square * kd + R[f"f{l}"][...])
    for c in range(3):
        start(0, c, R["r0"][c])
    run(0)
    backs = [
        pltpu.make_async_copy(
            R["x0"].at[:, :, pl.ds(v * nz, nz)], R["out"].at[v], R["lsem"].at[v]
        )
        for v in range(vecs)
    ]
    for one in backs:
        one.start()
    for one in backs:
        one.wait()


def chebyshev_table(spectrum, coef):
    for l in range(3):
        low, top = spectrum[l, 0], spectrum[l, 1]
        center = 0.5 * (top + low)
        radius = 0.5 * (top - low)
        ratio = center / radius
        rho = 1.0 / ratio
        steps = []
        for _ in range(COARSE_DEG - 1):
            rho_next = 1.0 / (2.0 * ratio - rho)
            steps.append((rho_next * rho, 2.0 * rho_next / radius))
            rho = rho_next
        smooth = steps[: DEG - 1]
        flat = [(0.0, 0.0), (0.0, 1.0 / center)]
        picked = steps if l == 2 else smooth + flat + smooth
        for k, two in enumerate(picked):
            coef[l, 2 * k] = jnp.asarray(two[0], F32)
            coef[l, 2 * k + 1] = jnp.asarray(two[1], F32)
        coef[l, 12] = 1.0 / center


def local(modes, moduli, pinned, spectrum):
    vecs, _, nx, ny, nz = modes.shape
    levels = []
    names, args = [], []

    def add(name, value):
        names.append(name)
        args.append(value)

    for l, degree in enumerate(DEGREES):
        step = DEGREES[0] // degree
        levels.append(Level(degree, nx // step, ny // step, nz // step, vecs))
    add("spectrum", spectrum)
    add("modes", modes.reshape(vecs, 3, nx * ny, nz))
    add("moduli_in", moduli.reshape(nx * ny, nz))
    add("pinned_in", pinned.reshape(nx * ny, nz))
    for l, lev in enumerate(levels):
        mats = dict(zip((f"wo{l}", f"wh{l}", f"z{l}"), lev.operator()))
        if l + 1 < len(levels):
            keys = [f"{a}{l}{b}" for a in ("rs", "pr") for b in "ohz"]
            mats.update(zip(keys, transfer(lev, levels[l + 1])))
        for key, mat in mats.items():
            for tag, half in zip("hl", split(mat)):
                add(key + tag + "_in", jnp.asarray(half))
        for key, mat in zip(("kr", "kl"), lev.diagonal()):
            add(f"{key}{l}_in", jnp.asarray(mat))
        if l or not lev.blocked:
            for key, mat in zip(("sx", "sz"), lev.sample(levels[0])):
                add(f"{key}{l}_in", jnp.asarray(mat.astype(BF16)))

    specs = [
        pl.BlockSpec(memory_space=pltpu.SMEM if n == "spectrum" else pl.ANY) for n in names
    ]
    scratch = []
    all_names = names + ["out"]

    def temp(name, what):
        all_names.append(name)
        scratch.append(what)

    temp("coef", pltpu.SMEM((3, 13), F32))
    temp("lsem", pltpu.SemaphoreType.DMA((len(names) + 2 * vecs,)))
    for name, value in zip(names, args):
        if name.endswith("_in"):
            shape = value.shape
            if name[:2] == "z0" and levels[0].blocked:
                shape = (shape[0], levels[0].lanes, levels[0].lanes)
            temp(name[:-3], pltpu.VMEM(shape, value.dtype))
    for l, lev in enumerate(levels):
        field = (3, lev.rows, lev.lanes)
        for n in ("s", "f"):
            temp(f"{n}{l}", pltpu.VMEM(field[1:], F32))
        for n in ("r", "d", "x", "work", "dinv"):
            temp(f"{n}{l}", pltpu.VMEM(field, F32))
        temp(f"prod{l}", pltpu.VMEM((3, 4 * lev.rows, lev.lanes), F32))
        temp(f"send{l}", pltpu.VMEM((3, lev.halo, lev.lanes), F32))
        temp(f"halo{l}", pltpu.VMEM((2, 3, lev.halo, lev.lanes), F32))
        temp(f"ssem{l}", pltpu.SemaphoreType.DMA((len(DIRS),)))
        temp(f"rsem{l}", pltpu.SemaphoreType.DMA((2, len(DIRS))))
    out = pl.pallas_call(
        functools.partial(kernel, levels, all_names),
        out_shape=jax.ShapeDtypeStruct((vecs, 3, nx * ny, nz), F32),
        in_specs=specs,
        out_specs=pl.BlockSpec(memory_space=pl.ANY),
        scratch_shapes=scratch,
        compiler_params=pltpu.CompilerParams(
            collective_id=0, has_side_effects=True, vmem_limit_bytes=60 * 1024 * 1024
        ),
    )(*args)
    return out.reshape(modes.shape)


def solution(mesh):
    placed = (P(None, None, "gx", "gy", None), P("gx", "gy", None), P("gx", "gy", None), P())
    return jax.shard_map(
        local,
        mesh=mesh,
        in_specs=placed,
        out_specs=P(None, None, "gx", "gy", None),
        check_vma=False,
    )
```
